8 devices in a mesh: pp: 4 (over z, y, x), ep: 2 (over core).
Axes of the slice: x: 2, y: 2, z: 1, core: 2. Of those that a mesh axis runs over, the one named last changes fastest.
Arguments:
- expert_out: bfloat16 [24, 8, 320, 4096], P('pp', 'ep')
- expert_ids: int32 [24, 2, 512, 2], P('pp', 'ep')
- slot_ids: int32 [24, 2, 512, 2], P('pp', 'ep')
- gate_vals: float32 [24, 2, 512, 2], P('pp', 'ep')
- residual: bfloat16 [24, 2, 512, 4096], P('pp', 'ep')
- norm_w: float32 [4, 4096], P('pp')
- w_query: bfloat16 [4, 4096, 32, 128], P('pp')
- w_key: bfloat16 [4, 4096, 32, 128], P('pp')
- w_value: bfloat16 [4, 4096, 32, 128], P('pp')
- w_out: bfloat16 [4, 32, 128, 4096], P('pp')
Outputs:
- output: bfloat16 [24, 2, 512, 4096], P('pp', 'ep')
All inputs are finite; a program needn't handle non-finite values.
Results may differ from the reference program's by a relative error of at most 0.0114582.
Values are sent between devices in bfloat16 or wider.
A program may use at most 1 GiB of HBM per device.

```python
import jax
import jax.numpy as jnp
from jax import lax

STAGES = 4
GROUP_SIZE = 2
NUM_MICRO = 6
SEQ_LEN = 512
SEQS_PER_DEV = 1
D_MODEL = 4096
NUM_EXPERTS = 8
TOP_K = 2
NUM_HEADS = 32
HEAD_DIM = 128
SRC_SLOTS = 160

TOKENS_DEV = SEQS_PER_DEV * SEQ_LEN
SEQS_ALL = GROUP_SIZE * SEQS_PER_DEV
CAPACITY = GROUP_SIZE * SRC_SLOTS
NUM_ROWS = STAGES * NUM_MICRO
QKV_WIDTH = NUM_HEADS * HEAD_DIM
NORM_EPS = 1e-6


def block_ranks(block_ids):
    perm_order = jnp.argsort(block_ids, stable=True)
    sorted_ids = block_ids[perm_order]
    group_start = jnp.searchsorted(sorted_ids, sorted_ids, side='left')
    rank_sorted = jnp.arange(block_ids.shape[0]) - group_start
    return jnp.zeros_like(block_ids).at[perm_order].set(rank_sorted)


def draw_routing(route_key):
    key_bias, key_hot, key_shift, key_noise, key_order = jax.random.split(route_key, 5)
    expert_bias = jnp.sum(jax.random.randint(key_bias, (NUM_ROWS, NUM_EXPERTS, 4), 0, 166, jnp.int32), axis=-1)
    hot_expert = jax.random.randint(key_hot, (NUM_ROWS,), 0, NUM_EXPERTS)
    cover_shift = jax.random.randint(key_shift, (NUM_ROWS,), 0, NUM_EXPERTS)
    local_pos = jnp.arange(TOKENS_DEV)
    expert_pos = jnp.arange(NUM_EXPERTS)
    tie_break = (NUM_EXPERTS - 1 - expert_pos).astype(jnp.int32)

    def one_block(flat_idx):
        row_idx = flat_idx // GROUP_SIZE
        blk_idx = flat_idx % GROUP_SIZE
        noise_draws = jnp.sum(jax.random.randint(jax.random.fold_in(key_noise, flat_idx), (TOKENS_DEV, NUM_EXPERTS, 3), 0, 164, jnp.int32), axis=-1)
        token_pos = blk_idx * TOKENS_DEV + local_pos
        is_cover = (token_pos[:, None] + cover_shift[row_idx]) % NUM_EXPERTS == expert_pos[None, :]
        is_hot = expert_pos[None, :] == hot_expert[row_idx]
        score_int = (expert_bias[row_idx][None, :] + noise_draws) * NUM_EXPERTS + tie_break[None, :] + (1 << 22) * is_cover.astype(jnp.int32) + (1 << 23) * is_hot.astype(jnp.int32)
        chosen = lax.top_k(score_int, TOP_K)[1]
        order_bits = jax.random.bits(jax.random.fold_in(key_order, flat_idx), (TOKENS_DEV, TOP_K), jnp.uint32) >> 8
        order_key = order_bits * TOP_K + jnp.arange(TOP_K, dtype=jnp.uint32)[None, :]
        perm_order = jnp.argsort(order_key, axis=1)
        chosen = jnp.take_along_axis(chosen, perm_order, axis=1)
        slot_rank = block_ranks(chosen.reshape(TOKENS_DEV * TOP_K)).reshape(TOKENS_DEV, TOP_K)
        slot_ids = jnp.where(slot_rank < SRC_SLOTS, blk_idx * SRC_SLOTS + slot_rank, -1)
        return chosen.astype(jnp.int32), slot_ids.astype(jnp.int32)

    expert_ids, slot_ids = lax.map(one_block, jnp.arange(NUM_ROWS * GROUP_SIZE))
    route_shape = (NUM_ROWS, SEQS_ALL, SEQ_LEN, TOP_K)
    return expert_ids.reshape(route_shape), slot_ids.reshape(route_shape)


def draw_bf16(draw_key, arr_shape, scale_fac):
    def one_slice(slice_key):
        return (scale_fac * jax.random.normal(slice_key, arr_shape[1:], jnp.float32)).astype(jnp.bfloat16)
    return lax.map(one_slice, jax.random.split(draw_key, arr_shape[0]))


def setup_inputs(seed: int = 0) -> dict:
    root_key = jax.random.key(seed)
    sub_keys = jax.random.split(root_key, 10)
    expert_ids, slot_ids = draw_routing(sub_keys[0])
    gate_vals = jax.nn.softmax(1.5 * jax.random.normal(sub_keys[1], (NUM_ROWS, SEQS_ALL, SEQ_LEN, TOP_K), jnp.float32), axis=-1)
    expert_scale = 1.5 * jnp.exp(0.5 * jax.random.normal(sub_keys[2], (NUM_ROWS * NUM_EXPERTS,), jnp.float32))

    def expert_slab(slab_args):
        slab_key, slab_scale = slab_args
        return (slab_scale * jax.random.normal(slab_key, (CAPACITY, D_MODEL), jnp.float32)).astype(jnp.bfloat16)

    expert_out = lax.map(expert_slab, (jax.random.split(sub_keys[3], NUM_ROWS * NUM_EXPERTS), expert_scale))
    expert_out = expert_out.reshape(NUM_ROWS, NUM_EXPERTS, CAPACITY, D_MODEL)
    residual = draw_bf16(sub_keys[4], (NUM_ROWS * SEQS_ALL, SEQ_LEN, D_MODEL), 1.0)
    residual = residual.reshape(NUM_ROWS, SEQS_ALL, SEQ_LEN, D_MODEL)
    norm_w = 1.0 + 0.4 * jax.random.normal(sub_keys[5], (STAGES, D_MODEL), jnp.float32)
    in_scale = D_MODEL ** -0.5
    out_scale = QKV_WIDTH ** -0.5
    w_query = draw_bf16(sub_keys[6], (STAGES, D_MODEL, NUM_HEADS, HEAD_DIM), 1.5 * in_scale)
    w_key = draw_bf16(sub_keys[7], (STAGES, D_MODEL, NUM_HEADS, HEAD_DIM), 1.5 * in_scale)
    w_value = draw_bf16(sub_keys[8], (STAGES, D_MODEL, NUM_HEADS, HEAD_DIM), in_scale)
    w_out = draw_bf16(sub_keys[9], (STAGES, NUM_HEADS, HEAD_DIM, D_MODEL), out_scale)
    return dict(expert_out=expert_out, expert_ids=expert_ids, slot_ids=slot_ids, gate_vals=gate_vals, residual=residual, norm_w=norm_w, w_query=w_query, w_key=w_key, w_value=w_value, w_out=w_out)


def reference(expert_out, expert_ids, slot_ids, gate_vals, residual, norm_w, w_query, w_key, w_value, w_out):
    causal = jnp.arange(SEQ_LEN)[:, None] >= jnp.arange(SEQ_LEN)[None, :]

    def one_stage(stage_idx):
        src_stage = (stage_idx + STAGES - 1) % STAGES
        stage_norm = norm_w[stage_idx]
        stage_wq = w_query[stage_idx].reshape(D_MODEL, QKV_WIDTH)
        stage_wk = w_key[stage_idx].reshape(D_MODEL, QKV_WIDTH)
        stage_wv = w_value[stage_idx].reshape(D_MODEL, QKV_WIDTH)
        stage_wo = w_out[stage_idx].reshape(QKV_WIDTH, D_MODEL)

        def project(x_in, weight_mat):
            head_out = jnp.dot(x_in, weight_mat, preferred_element_type=jnp.float32).astype(jnp.bfloat16)
            return head_out.reshape(SEQ_LEN, NUM_HEADS, HEAD_DIM).astype(jnp.float32)

        def one_sequence(flat_idx):
            src_row = src_stage * NUM_MICRO + flat_idx // SEQS_ALL
            seq_idx = flat_idx % SEQS_ALL
            ids_seq = expert_ids[src_row, seq_idx]
            slot_seq = slot_ids[src_row, seq_idx]
            is_kept = slot_seq >= 0
            picked = expert_out[src_row, ids_seq, jnp.where(is_kept, slot_seq, 0)].astype(jnp.float32)
            weight = jnp.where(is_kept, gate_vals[src_row, seq_idx], 0.0)
            mixed_sum = residual[src_row, seq_idx].astype(jnp.float32) + jnp.sum(weight[:, :, None] * picked, axis=1)
            y_wide = mixed_sum.astype(jnp.bfloat16).astype(jnp.float32)
            inv_rms = lax.rsqrt(jnp.mean(y_wide * y_wide, axis=-1, keepdims=True) + NORM_EPS)
            x_in = (y_wide * inv_rms * stage_norm).astype(jnp.bfloat16)
            q_heads = project(x_in, stage_wq)
            k_heads = project(x_in, stage_wk)
            v_heads = project(x_in, stage_wv)
            scores = jnp.einsum('qhe,khe->hqk', q_heads, k_heads) * HEAD_DIM ** -0.5
            attn_probs = jax.nn.softmax(jnp.where(causal, scores, -jnp.inf), axis=-1).astype(jnp.bfloat16)
            attn_out = jnp.einsum('hqk,khe->qhe', attn_probs.astype(jnp.float32), v_heads).astype(jnp.bfloat16)
            out_proj = jnp.dot(attn_out.reshape(SEQ_LEN, QKV_WIDTH), stage_wo, preferred_element_type=jnp.float32).astype(jnp.bfloat16)
            return (y_wide + out_proj.astype(jnp.float32)).astype(jnp.bfloat16)

        return lax.map(one_sequence, jnp.arange(NUM_MICRO * SEQS_ALL))

    stage_outs = lax.map(one_stage, jnp.arange(STAGES))
    return stage_outs.reshape(NUM_ROWS, SEQS_ALL, SEQ_LEN, D_MODEL)
```

```python
import functools

import jax
import jax.numpy as jnp
from jax import lax
from jax.experimental import pallas as pl
from jax.experimental.pallas import tpu as pltpu
from jax.sharding import PartitionSpec as P


NORM_EPS = 1e-6
LOG2E = 1.4426950408889634
LANES = 128


def combine_kernel(micros, key_ref, gate_ref, expert_ref, res_ref, *refs):
    count = len(micros)
    out_refs = refs[:count]
    table_ref, pick_ref, wide_ref, own_sem, send_sem, recv_sem = refs[count:]
    tiles = table_ref.shape[0] // count
    experts, src_slots, width = table_ref.shape[1] // 2, table_ref.shape[2], table_ref.shape[3]
    num_rows, depth = pick_ref.shape
    tokens = num_rows // 2
    step, tile = pl.program_id(0), pl.program_id(1)
    slot = step * tiles + tile
    me = lax.axis_index('ep')
    mate = 1 - me

    def own_rows(step, tile, slot):
        cols = pl.ds(pl.multiple_of(tile * width, width), width)
        rows = pl.ds(pl.multiple_of(me * src_slots, src_slots), src_slots)
        return pltpu.make_async_copy(expert_ref.at[micros[0] + step, :, rows, cols], table_ref.at[slot, :experts], own_sem.at[slot])

    def mate_rows(step, tile, slot):
        cols = pl.ds(pl.multiple_of(tile * width, width), width)
        rows = pl.ds(pl.multiple_of(mate * src_slots, src_slots), src_slots)
        return pltpu.make_async_remote_copy(
            src_ref=expert_ref.at[micros[0] + step, :, rows, cols],
            dst_ref=table_ref.at[slot, experts:],
            send_sem=send_sem.at[slot],
            recv_sem=recv_sem.at[slot],
            device_id={'ep': mate},
            device_id_type=pl.DeviceIdType.MESH,
        )

    @pl.when(slot == 0)
    def _():
        barrier = pltpu.get_barrier_semaphore()
        pl.semaphore_signal(barrier, inc=1, device_id={'ep': mate}, device_id_type=pl.DeviceIdType.MESH)
        for at in range(min(2, tiles * count)):
            own_rows(at // tiles, at % tiles, at).start()
        pl.semaphore_wait(barrier, 1)

        def launch(at, carry):
            mate_rows(at // tiles, at % tiles, at).start()

            @pl.when(at >= 2)
            def _():
                own_rows(at // tiles, at % tiles, at).start()

            return carry

        lax.fori_loop(0, tiles * count, launch, 0)

    @pl.when(tile == 0)
    def _():
        for choice in range(2):
            rows = slice(choice * tokens, (choice + 1) * tokens)
            wide_ref[rows] = jnp.broadcast_to(gate_ref[0, choice:choice + 1, :], (LANES, tokens)).T
            keys = jnp.broadcast_to(key_ref[0, choice:choice + 1, :], (LANES, tokens)).T
            lane = lax.broadcasted_iota(jnp.int32, keys.shape, 1)
            for col in range(0, depth, LANES):
                pick_ref[rows, col:col + LANES] = jnp.where(keys == lane + col, 1.0, 0.0).astype(pick_ref.dtype)

    own_rows(step, tile, slot).wait()
    arriving = mate_rows(step, tile, slot)
    arriving.wait_recv()
    table = table_ref[slot].reshape(depth, width)
    picked = jnp.dot(pick_ref[...], table, preferred_element_type=jnp.float32)
    first, second = wide_ref[:tokens], wide_ref[tokens:]
    mixed = []
    for col in range(0, width, LANES):
        cols = slice(col, col + LANES)
        gated = first * picked[:tokens, cols] + second * picked[tokens:, cols]
        mixed.append((res_ref[0, 0, :, cols].astype(jnp.float32) + gated).astype(jnp.bfloat16))
    mixed = jnp.concatenate(mixed, axis=1)
    for at, out_ref in enumerate(out_refs):
        @pl.when(step == at)
        def _(out_ref=out_ref):
            out_ref[...] = mixed
    arriving.wait_send()


def combine(micros, call_id, keys, gates, expert_out, residual, width):
    _, experts, capacity, d_model = expert_out.shape
    src_slots = capacity // 2
    tokens = residual.shape[2]
    depth = 2 * experts * src_slots
    count, tiles, base = len(micros), d_model // width, micros[0]

    def out_spec(at):
        return pl.BlockSpec((tokens, width), lambda m, n: (0, jnp.where(m < at, 0, jnp.where(m > at, tiles - 1, n))))

    return pl.pallas_call(
        functools.partial(combine_kernel, micros),
        out_shape=[jax.ShapeDtypeStruct((tokens, d_model), jnp.bfloat16)] * count,
        grid=(count, tiles),
        in_specs=[
            pl.BlockSpec((1, 2, tokens), lambda m, n: (base + m, 0, 0)),
            pl.BlockSpec((1, 2, tokens), lambda m, n: (base + m, 0, 0)),
            pl.BlockSpec(memory_space=pl.ANY),
            pl.BlockSpec((1, 1, tokens, width), lambda m, n: (base + m, 0, 0, n)),
        ],
        out_specs=[out_spec(at) for at in range(count)],
        scratch_shapes=[
            pltpu.VMEM((count * tiles, 2 * experts, src_slots, width), jnp.bfloat16),
            pltpu.VMEM((2 * tokens, depth), jnp.bfloat16),
            pltpu.VMEM((2 * tokens, LANES), jnp.float32),
            pltpu.SemaphoreType.DMA((count * tiles,)),
            pltpu.SemaphoreType.DMA((count * tiles,)),
            pltpu.SemaphoreType.DMA((count * tiles,)),
        ],
        compiler_params=pltpu.CompilerParams(vmem_limit_bytes=60 << 20, collective_id=call_id, has_side_effects=True),
        cost_estimate=pl.CostEstimate(flops=4 * count * tokens * depth * d_model, bytes_accessed=2 * count * d_model * (depth + 2 * tokens), transcendentals=0),
        name='combine',
    )(keys, gates, expert_out, residual)


def regroup_kernel(wt_ref, out_ref, wide_ref):
    rows, heads, head_dim = wt_ref.shape[1:]
    wide_ref[...] = wt_ref[0].astype(jnp.float32).reshape(rows * heads, head_dim)
    for head in range(heads):
        out_ref[:, head * head_dim:(head + 1) * head_dim] = wide_ref[pl.ds(head, rows, stride=heads), :].astype(out_ref.dtype)


def regroup(weight, rows, heads):
    _, d_model, num_heads, head_dim = weight.shape
    return pl.pallas_call(
        regroup_kernel,
        out_shape=jax.ShapeDtypeStruct((d_model, num_heads * head_dim), weight.dtype),
        grid=(d_model // rows, num_heads // heads),
        in_specs=[pl.BlockSpec((1, rows, heads, head_dim), lambda r, h: (0, r, h, 0))],
        out_specs=pl.BlockSpec((rows, heads * head_dim), lambda r, h: (r, h)),
        scratch_shapes=[pltpu.VMEM((rows * heads, head_dim), jnp.float32)],
        compiler_params=pltpu.CompilerParams(vmem_limit_bytes=32 << 20),
        cost_estimate=pl.CostEstimate(flops=10 ** 10, bytes_accessed=4 * d_model * num_heads * head_dim, transcendentals=0),
        name='regroup',
    )(weight)


def attention_kernel(y_ref, norm_ref, wq_ref, wk_ref, wv_ref, out_ref, x_ref, q_ref, k_ref, v_ref):
    seq_len, _ = y_ref.shape
    head_dim = LANES
    block = seq_len // 2

    @pl.when(pl.program_id(0) == 0)
    def _():
        strip = 32

        def norm_strip(step, carry):
            rows = pl.ds(pl.multiple_of(step * strip, strip), strip)
            y_wide = y_ref[rows, :].astype(jnp.float32)
            inv_rms = lax.rsqrt(jnp.mean(y_wide * y_wide, axis=-1, keepdims=True) + NORM_EPS)
            x_ref[rows, :] = (y_wide * inv_rms * norm_ref[...]).astype(x_ref.dtype)
            return carry

        lax.fori_loop(0, seq_len // strip, norm_strip, 0)

    for wt_ref, dst_ref in ((wq_ref, q_ref), (wk_ref, k_ref), (wv_ref, v_ref)):
        dst_ref[...] = jnp.dot(x_ref[...], wt_ref[...], preferred_element_type=jnp.float32).astype(dst_ref.dtype)

    factor = (head_dim ** -0.5) * LOG2E
    row_pos = lax.broadcasted_iota(jnp.int32, (block, block), 0)
    col_pos = lax.broadcasted_iota(jnp.int32, (block, block), 1)
    seen = row_pos >= col_pos
    contract = (((1,), (1,)), ((), ()))
    for head in range(out_ref.shape[1] // head_dim):
        cols = slice(head * head_dim, (head + 1) * head_dim)
        for part in range(2):
            rows = slice(part * block, (part + 1) * block)
            query = q_ref[rows, cols]
            pieces = []
            if part:
                pieces.append(lax.dot_general(query, k_ref[:block, cols], contract, preferred_element_type=jnp.float32))
            last = lax.dot_general(query, k_ref[rows, cols], contract, preferred_element_type=jnp.float32)
            pieces.append(jnp.where(seen, last, -jnp.inf))
            scores = jnp.concatenate(pieces, axis=1) if part else pieces[0]
            top = jnp.max(scores, axis=1, keepdims=True)
            grown = jnp.exp2((scores - top) * factor)
            probs = (grown * (1.0 / jnp.sum(grown, axis=1, keepdims=True))).astype(jnp.bfloat16)
            mixed = jnp.dot(probs, v_ref[:(part + 1) * block, cols], preferred_element_type=jnp.float32)
            out_ref[rows, cols] = mixed.astype(out_ref.dtype)


def attention(arrived, norm_w, weights, width):
    seq_len, d_model = arrived.shape
    depth = weights[0].shape[1]
    wt_spec = pl.BlockSpec((d_model, width), lambda h: (0, h))
    head_scratch = pltpu.VMEM((seq_len, width), jnp.bfloat16)
    return pl.pallas_call(
        attention_kernel,
        out_shape=jax.ShapeDtypeStruct((seq_len, depth), jnp.bfloat16),
        grid=(depth // width,),
        in_specs=[
            pl.BlockSpec((seq_len, d_model), lambda h: (0, 0)),
            pl.BlockSpec((1, d_model), lambda h: (0, 0)),
            wt_spec, wt_spec, wt_spec,
        ],
        out_specs=pl.BlockSpec((seq_len, width), lambda h: (0, h)),
        scratch_shapes=[pltpu.VMEM((seq_len, d_model), jnp.bfloat16), head_scratch, head_scratch, head_scratch],
        compiler_params=pltpu.CompilerParams(vmem_limit_bytes=60 << 20),
        cost_estimate=pl.CostEstimate(flops=6 * seq_len * d_model * depth, bytes_accessed=6 * d_model * depth, transcendentals=0),
        name='attention',
    )(arrived, norm_w, *weights)


def project_kernel(attn_ref, wt_ref, res_ref, *refs):
    out_ref = refs[-1]
    proj = jnp.dot(attn_ref[...], wt_ref[...], preferred_element_type=jnp.float32).astype(jnp.bfloat16)
    out_ref[0, 0] = (res_ref[...].astype(jnp.float32) + proj.astype(jnp.float32)).astype(out_ref.dtype)


def project(micro, attn_out, w_out, arrived, result, out_shape, tile):
    tokens, depth = attn_out.shape
    d_model = w_out.shape[1]
    in_specs = [
        pl.BlockSpec((tokens, depth), lambda n: (0, 0)),
        pl.BlockSpec((depth, tile), lambda n: (0, n)),
        pl.BlockSpec((tokens, tile), lambda n: (0, n)),
    ]
    operands = [attn_out, w_out, arrived]
    aliases = {}
    if result is not None:
        in_specs.append(pl.BlockSpec(memory_space=pl.ANY))
        operands.append(result)
        aliases = {3: 0}
    return pl.pallas_call(
        project_kernel,
        out_shape=jax.ShapeDtypeStruct(out_shape, jnp.bfloat16),
        grid=(d_model // tile,),
        in_specs=in_specs,
        out_specs=pl.BlockSpec((1, 1, tokens, tile), lambda n: (micro, 0, 0, n)),
        input_output_aliases=aliases,
        compiler_params=pltpu.CompilerParams(vmem_limit_bytes=60 << 20),
        cost_estimate=pl.CostEstimate(flops=2 * tokens * depth * d_model, bytes_accessed=2 * depth * d_model, transcendentals=0),
        name='project',
    )(*operands)


def solution(mesh):
    stages = mesh.shape['pp']
    group_size = mesh.shape['ep']
    send_next = [(src, (src + 1) % stages) for src in range(stages)]
    tok_spec = P('pp', 'ep', None, None)
    wt_spec = P('pp', None, None, None)

    def device_step(expert_out, expert_ids, slot_ids, gate_vals, residual, norm_w, w_query, w_key, w_value, w_out):
        num_micro, _, _, d_model = residual.shape
        experts, capacity = expert_out.shape[1:3]
        src_slots = capacity // group_size
        num_experts = experts * group_size
        position = lax.axis_index('ep').astype(jnp.int32)

        place = (expert_ids[:, 0] - position * experts) % num_experts
        keys = jnp.where(slot_ids[:, 0] >= 0, place * src_slots + slot_ids[:, 0] - position * src_slots, -1)
        keys = jnp.swapaxes(keys, 1, 2)
        gates = jnp.swapaxes(gate_vals[:, 0], 1, 2)

        arrived = []
        combined = []
        for call_id, micros in enumerate(((0,), (1, 2), (3, 4, 5))):
            if combined:
                keys = lax.optimization_barrier((keys, combined[-1]))[0]
            rows = combine(micros, call_id, keys, gates, expert_out, residual, 512)
            combined.extend(rows)
            for micro, row in zip(micros, rows):
                arrived.append(lax.ppermute(row, 'pp', send_next))
        raw = lax.optimization_barrier((w_query, w_key, w_value, combined[-1]))[:3]
        weights = [regroup(wt, 256, 8) for wt in raw]

        flat_out = w_out[0].reshape(-1, d_model)
        result = None
        for micro in range(num_micro):
            rows = arrived[micro]
            if micro:
                rows, result = lax.optimization_barrier((rows, result))
            attn_out = attention(rows, norm_w, weights, 512)
            result = project(micro, attn_out, flat_out, rows, result, residual.shape, 512)
        return result

    return jax.shard_map(device_step, mesh=mesh, in_specs=(tok_spec, tok_spec, tok_spec, tok_spec, tok_spec, P('pp', None), wt_spec, wt_spec, wt_spec, wt_spec), out_specs=tok_spec, check_vma=False)
```

```python
import functools

import jax
import jax.numpy as jnp
from jax import lax
from jax.experimental import pallas as pl
from jax.experimental.pallas import tpu as pltpu
from jax.sharding import PartitionSpec as P


NORM_EPS = 1e-6
LOG2E = 1.4426950408889634
LANES = 128


def combine_kernel(micros, key_ref, gate_ref, expert_ref, res_ref, *refs):
    count = len(micros)
    out_refs = refs[:count]
    table_ref, pick_ref, wide_ref, own_sem, send_sem, recv_sem = refs[count:]
    tiles = table_ref.shape[0] // count
    experts, src_slots, width = table_ref.shape[1] // 2, table_ref.shape[2], table_ref.shape[3]
    num_rows, depth = pick_ref.shape
    tokens = num_rows // 2
    step, tile = pl.program_id(0), pl.program_id(1)
    slot = step * tiles + tile
    me = lax.axis_index('ep')
    mate = 1 - me

    def own_rows(step, tile, slot):
        cols = pl.ds(pl.multiple_of(tile * width, width), width)
        rows = pl.ds(pl.multiple_of(me * src_slots, src_slots), src_slots)
        return pltpu.make_async_copy(expert_ref.at[micros[0] + step, :, rows, cols], table_ref.at[slot, :experts], own_sem.at[slot])

    def mate_rows(step, tile, slot):
        cols = pl.ds(pl.multiple_of(tile * width, width), width)
        rows = pl.ds(pl.multiple_of(mate * src_slots, src_slots), src_slots)
        return pltpu.make_async_remote_copy(
            src_ref=expert_ref.at[micros[0] + step, :, rows, cols],
            dst_ref=table_ref.at[slot, experts:],
            send_sem=send_sem.at[slot],
            recv_sem=recv_sem.at[slot],
            device_id={'ep': mate},
            device_id_type=pl.DeviceIdType.MESH,
        )

    @pl.when(slot == 0)
    def _():
        barrier = pltpu.get_barrier_semaphore()
        pl.semaphore_signal(barrier, inc=1, device_id={'ep': mate}, device_id_type=pl.DeviceIdType.MESH)
        for at in range(min(2, tiles * count)):
            own_rows(at // tiles, at % tiles, at).start()
        pl.semaphore_wait(barrier, 1)

        def launch(at, carry):
            mate_rows(at // tiles, at % tiles, at).start()

            @pl.when(at >= 2)
            def _():
                own_rows(at // tiles, at % tiles, at).start()

            return carry

        lax.fori_loop(0, tiles * count, launch, 0)

    @pl.when(tile == 0)
    def _():
        for choice in range(2):
            rows = slice(choice * tokens, (choice + 1) * tokens)
            wide_ref[rows] = jnp.broadcast_to(gate_ref[0, choice:choice + 1, :], (LANES, tokens)).T
            keys = jnp.broadcast_to(key_ref[0, choice:choice + 1, :], (LANES, tokens)).T
            lane = lax.broadcasted_iota(jnp.int32, keys.shape, 1)
            for col in range(0, depth, LANES):
                pick_ref[rows, col:col + LANES] = jnp.where(keys == lane + col, 1.0, 0.0).astype(pick_ref.dtype)

    own_rows(step, tile, slot).wait()
    arriving = mate_rows(step, tile, slot)
    arriving.wait_recv()
    table = table_ref[slot].reshape(depth, width)
    picked = jnp.dot(pick_ref[...], table, preferred_element_type=jnp.float32)
    first, second = wide_ref[:tokens], wide_ref[tokens:]
    mixed = []
    for col in range(0, width, LANES):
        cols = slice(col, col + LANES)
        gated = first * picked[:tokens, cols] + second * picked[tokens:, cols]
        mixed.append((res_ref[0, 0, :, cols].astype(jnp.float32) + gated).astype(jnp.bfloat16))
    mixed = jnp.concatenate(mixed, axis=1)
    for at, out_ref in enumerate(out_refs):
        @pl.when(step == at)
        def _(out_ref=out_ref):
            out_ref[...] = mixed
    arriving.wait_send()


def combine(micros, call_id, keys, gates, expert_out, residual, width):
    _, experts, capacity, d_model = expert_out.shape
    src_slots = capacity // 2
    tokens = residual.shape[2]
    depth = 2 * experts * src_slots
    count, tiles, base = len(micros), d_model // width, micros[0]

    def out_spec(at):
        return pl.BlockSpec((tokens, width), lambda m, n: (0, jnp.where(m < at, 0, jnp.where(m > at, tiles - 1, n))))

    return pl.pallas_call(
        functools.partial(combine_kernel, micros),
        out_shape=[jax.ShapeDtypeStruct((tokens, d_model), jnp.bfloat16)] * count,
        grid=(count, tiles),
        in_specs=[
            pl.BlockSpec((1, 2, tokens), lambda m, n: (base + m, 0, 0)),
            pl.BlockSpec((1, 2, tokens), lambda m, n: (base + m, 0, 0)),
            pl.BlockSpec(memory_space=pl.ANY),
            pl.BlockSpec((1, 1, tokens, width), lambda m, n: (base + m, 0, 0, n)),
        ],
        out_specs=[out_spec(at) for at in range(count)],
        scratch_shapes=[
            pltpu.VMEM((count * tiles, 2 * experts, src_slots, width), jnp.bfloat16),
            pltpu.VMEM((2 * tokens, depth), jnp.bfloat16),
            pltpu.VMEM((2 * tokens, LANES), jnp.float32),
            pltpu.SemaphoreType.DMA((count * tiles,)),
            pltpu.SemaphoreType.DMA((count * tiles,)),
            pltpu.SemaphoreType.DMA((count * tiles,)),
        ],
        compiler_params=pltpu.CompilerParams(vmem_limit_bytes=60 << 20, collective_id=call_id, has_side_effects=True),
        cost_estimate=pl.CostEstimate(flops=4 * count * tokens * depth * d_model, bytes_accessed=2 * count * d_model * (depth + 2 * tokens), transcendentals=0),
        name='combine',
    )(keys, gates, expert_out, residual)


def regroup_kernel(wt_ref, out_ref, wide_ref):
    heads, head_dim = wt_ref.shape[2:]
    strip = wide_ref.shape[0] // heads

    def regroup_strip(at, carry):
        rows = pl.ds(pl.multiple_of(at * strip, strip), strip)
        wide_ref[...] = wt_ref[0, rows].astype(jnp.float32).reshape(strip * heads, head_dim)
        for head in range(heads):
            out_ref[rows, head * head_dim:(head + 1) * head_dim] = wide_ref[pl.ds(head, strip, stride=heads), :].astype(out_ref.dtype)
        return carry

    lax.fori_loop(0, wt_ref.shape[1] // strip, regroup_strip, 0)


def regroup(weight, rows, heads):
    _, d_model, num_heads, head_dim = weight.shape
    return pl.pallas_call(
        regroup_kernel,
        out_shape=jax.ShapeDtypeStruct((d_model, num_heads * head_dim), weight.dtype),
        grid=(d_model // rows, num_heads // heads),
        in_specs=[pl.BlockSpec((1, rows, heads, head_dim), lambda r, h: (0, r, h, 0))],
        out_specs=pl.BlockSpec((rows, heads * head_dim), lambda r, h: (r, h)),
        scratch_shapes=[pltpu.VMEM((128 * heads, head_dim), jnp.float32)],
        compiler_params=pltpu.CompilerParams(vmem_limit_bytes=32 << 20),
        cost_estimate=pl.CostEstimate(flops=10 ** 10, bytes_accessed=4 * d_model * num_heads * head_dim, transcendentals=0),
        name='regroup',
    )(weight)


def attend(q_ref, k_ref, v_ref, head, part):
    seq_len, head_dim = q_ref.shape[0], LANES
    block = seq_len // 2
    cols = slice(head * head_dim, (head + 1) * head_dim)
    rows = slice(part * block, (part + 1) * block)
    contract = (((1,), (1,)), ((), ()))
    query = q_ref[rows, cols]
    seen = lax.broadcasted_iota(jnp.int32, (block, block), 0) >= lax.broadcasted_iota(jnp.int32, (block, block), 1)
    last = lax.dot_general(query, k_ref[rows, cols], contract, preferred_element_type=jnp.float32)
    scores = jnp.where(seen, last, -jnp.inf)
    if part:
        early = lax.dot_general(query, k_ref[:block, cols], contract, preferred_element_type=jnp.float32)
        scores = jnp.concatenate([early, scores], axis=1)
    top = jnp.max(scores, axis=1, keepdims=True)
    grown = jnp.exp2((scores - top) * ((head_dim ** -0.5) * LOG2E))
    probs = (grown * (1.0 / jnp.sum(grown, axis=1, keepdims=True))).astype(jnp.bfloat16)
    mixed = jnp.dot(probs, v_ref[:(part + 1) * block, cols], preferred_element_type=jnp.float32)
    return rows, mixed.astype(jnp.bfloat16)


def attention_kernel(norm_ref, y_hbm, wq_hbm, wk_hbm, wv_hbm, wo_hbm, *refs):
    (out_ref, y_ref, x_ref, attn_ref, wt_ref, wo_ref, qa_ref, ka_ref, va_ref, qb_ref, kb_ref, vb_ref, y_sem, wt_sem, wo_sem) = refs[-15:]
    seq_len, d_model = y_ref.shape
    width = wt_ref.shape[3]
    pair = width // 2
    steps = wq_hbm.shape[1] // width
    tile = wo_ref.shape[2]
    step = pl.program_id(0)

    def wt_copies(at):
        cols = pl.ds(pl.multiple_of(at * width, width), width)
        return [pltpu.make_async_copy(hbm.at[:, cols], wt_ref.at[at % 2, which], wt_sem.at[at % 2, which]) for which, hbm in enumerate((wq_hbm, wk_hbm, wv_hbm))]

    def wo_copy(at):
        cols = pl.ds(pl.multiple_of(at * tile, tile), tile)
        return pltpu.make_async_copy(wo_hbm.at[:, cols], wo_ref.at[at % 2], wo_sem.at[at % 2])

    @pl.when(step == 0)
    def _():
        y_copy = pltpu.make_async_copy(y_hbm, y_ref, y_sem)
        y_copy.start()
        for copy in wt_copies(0):
            copy.start()
        y_copy.wait()
        strip = 32

        def norm_strip(at, carry):
            rows = pl.ds(pl.multiple_of(at * strip, strip), strip)
            y_wide = y_ref[rows, :].astype(jnp.float32)
            inv_rms = lax.rsqrt(jnp.mean(y_wide * y_wide, axis=-1, keepdims=True) + NORM_EPS)
            x_ref[rows, :] = (y_wide * inv_rms * norm_ref[...]).astype(x_ref.dtype)
            return carry

        lax.fori_loop(0, seq_len // strip, norm_strip, 0)
        for ref in (qb_ref, kb_ref, vb_ref):
            ref[...] = jnp.zeros_like(ref)

    @pl.when(step < steps)
    def _():
        @pl.when(step < steps - 1)
        def _():
            for copy in wt_copies(step + 1):
                copy.start()

        @pl.when(step == steps - 1)
        def _():
            wo_copy(0).start()

        for copy in wt_copies(step):
            copy.wait()
        slot = step % 2

        def emit(dst_refs, half, src_refs, base):
            for which, dst_ref in enumerate(dst_refs):
                wt = wt_ref[slot, which, :, half * pair:(half + 1) * pair]
                dst_ref[...] = jnp.dot(x_ref[...], wt, preferred_element_type=jnp.float32).astype(dst_ref.dtype)
                if which < 2:
                    for part in range(2):
                        rows, mixed = attend(*src_refs, which, part)
                        attn_ref[rows, pl.ds(pl.multiple_of(base + which * LANES, LANES), LANES)] = mixed

        first, second = (qa_ref, ka_ref, va_ref), (qb_ref, kb_ref, vb_ref)
        before = jnp.where(step == 0, steps - 1, step - 1)
        emit(first, 0, second, before * width + pair)
        emit(second, 1, first, step * width)

    @pl.when(step == steps)
    def _():
        for head in range(2):
            for part in range(2):
                rows, mixed = attend(qb_ref, kb_ref, vb_ref, head, part)
                at = attn_ref.shape[1] - pair + head * LANES
                attn_ref[rows, at:at + LANES] = mixed

    @pl.when(step >= steps)
    def _():
        at = step - steps

        @pl.when(at + 1 < d_model // tile)
        def _():
            wo_copy(at + 1).start()

        wo_copy(at).wait()
        proj = jnp.dot(attn_ref[...], wo_ref[at % 2], preferred_element_type=jnp.float32).astype(jnp.bfloat16)
        y_tile = y_ref[:, pl.ds(pl.multiple_of(at * tile, tile), tile)]
        out_ref[0, 0] = (y_tile.astype(jnp.float32) + proj.astype(jnp.float32)).astype(out_ref.dtype)


def attention(micro, arrived, norm_w, weights, w_out, result, out_shape, width, tile):
    seq_len, d_model = arrived.shape
    depth = weights[0].shape[1]
    steps = depth // width
    hbm = pl.BlockSpec(memory_space=pl.ANY)
    operands = [norm_w, arrived, *weights, w_out]
    aliases = {}
    if result is not None:
        operands.append(result)
        aliases = {len(operands) - 1: 0}
    head_pair = pltpu.VMEM((seq_len, width // 2), jnp.bfloat16)
    return pl.pallas_call(
        attention_kernel,
        out_shape=jax.ShapeDtypeStruct(out_shape, jnp.bfloat16),
        grid=(steps + d_model // tile,),
        in_specs=[pl.BlockSpec((1, d_model), lambda h: (0, 0))] + [hbm] * (len(operands) - 1),
        out_specs=pl.BlockSpec((1, 1, seq_len, tile), lambda h: (micro, 0, 0, jnp.maximum(h - steps, 0))),
        scratch_shapes=[
            pltpu.VMEM((seq_len, d_model), jnp.bfloat16),
            pltpu.VMEM((seq_len, d_model), jnp.bfloat16),
            pltpu.VMEM((seq_len, depth), jnp.bfloat16),
            pltpu.VMEM((2, 3, d_model, width), jnp.bfloat16),
            pltpu.VMEM((2, depth, tile), jnp.bfloat16),
            *[head_pair] * 6,
            pltpu.SemaphoreType.DMA,
            pltpu.SemaphoreType.DMA((2, 3)),
            pltpu.SemaphoreType.DMA((2,)),
        ],
        input_output_aliases=aliases,
        compiler_params=pltpu.CompilerParams(vmem_limit_bytes=60 << 20),
        cost_estimate=pl.CostEstimate(flops=8 * seq_len * d_model * depth, bytes_accessed=8 * d_model * depth, transcendentals=0),
        name='attention',
    )(*operands)


def solution(mesh):
    stages = mesh.shape['pp']
    group_size = mesh.shape['ep']
    send_next = [(src, (src + 1) % stages) for src in range(stages)]
    tok_spec = P('pp', 'ep', None, None)
    wt_spec = P('pp', None, None, None)

    def device_step(expert_out, expert_ids, slot_ids, gate_vals, residual, norm_w, w_query, w_key, w_value, w_out):
        num_micro, _, _, d_model = residual.shape
        experts, capacity = expert_out.shape[1:3]
        src_slots = capacity // group_size
        num_experts = experts * group_size
        position = lax.axis_index('ep').astype(jnp.int32)

        place = (expert_ids[:, 0] - position * experts) % num_experts
        keys = jnp.where(slot_ids[:, 0] >= 0, place * src_slots + slot_ids[:, 0] - position * src_slots, -1)
        keys = jnp.swapaxes(keys, 1, 2)
        gates = jnp.swapaxes(gate_vals[:, 0], 1, 2)

        arrived = []
        combined = []
        for call_id, micros in enumerate(((0,), (1, 2), (3, 4, 5))):
            if combined:
                keys = lax.optimization_barrier((keys, combined[-1]))[0]
            rows = combine(micros, call_id, keys, gates, expert_out, residual, 512)
            combined.extend(rows)
            for micro, row in zip(micros, rows):
                arrived.append(lax.ppermute(row, 'pp', send_next))
        raw = lax.optimization_barrier((w_query, w_key, w_value, combined[-1]))[:3]
        weights = [regroup(wt, 1024, 8) for wt in raw]

        flat_out = w_out[0].reshape(-1, d_model)
        result = None
        for micro in range(num_micro):
            rows = arrived[micro]
            if micro:
                rows, result = lax.optimization_barrier((rows, result))
            result = attention(micro, rows, norm_w, weights, flat_out, result, residual.shape, 512, 512)
        return result

    return jax.shard_map(device_step, mesh=mesh, in_specs=(tok_spec, tok_spec, tok_spec, tok_spec, tok_spec, P('pp', None), wt_spec, wt_spec, wt_spec, wt_spec), out_specs=tok_spec, check_vma=False)
```

```python
import functools

import jax
import jax.numpy as jnp
from jax import lax
from jax.experimental import pallas as pl
from jax.experimental.pallas import tpu as pltpu
from jax.sharding import PartitionSpec as P


NORM_EPS = 1e-6
LOG2E = 1.4426950408889634
LANES = 128


def combine_kernel(micros, key_ref, gate_ref, expert_ref, res_ref, *refs):
    count = len(micros)
    out_refs = refs[:count]
    table_ref, pick_ref, wide_ref, own_sem, send_sem, recv_sem = refs[count:]
    slots = table_ref.shape[0]
    experts, src_slots, span = table_ref.shape[1] // 2, table_ref.shape[2], table_ref.shape[3]
    halves, tokens, width = slots // count, out_refs[0].shape[0], out_refs[0].shape[1]
    per_slot = span // width
    depth = pick_ref.shape[1]
    block = tokens // 2
    step, tile = pl.program_id(0), pl.program_id(1)
    slot = step * halves + tile // per_slot
    me = lax.axis_index('ep')
    mate = 1 - me

    def own_rows(slot):
        cols = pl.ds(pl.multiple_of(slot % halves * span, span), span)
        rows = pl.ds(pl.multiple_of(me * src_slots, src_slots), src_slots)
        return pltpu.make_async_copy(expert_ref.at[micros[0] + slot // halves, :, rows, cols], table_ref.at[slot, :experts], own_sem.at[slot])

    def mate_rows(slot):
        cols = pl.ds(pl.multiple_of(slot % halves * span, span), span)
        rows = pl.ds(pl.multiple_of(mate * src_slots, src_slots), src_slots)
        return pltpu.make_async_remote_copy(
            src_ref=expert_ref.at[micros[0] + slot // halves, :, rows, cols],
            dst_ref=table_ref.at[slot, experts:],
            send_sem=send_sem.at[slot],
            recv_sem=recv_sem.at[slot],
            device_id={'ep': mate},
            device_id_type=pl.DeviceIdType.MESH,
        )

    @pl.when((step == 0) & (tile == 0))
    def _():
        barrier = pltpu.get_barrier_semaphore()
        pl.semaphore_signal(barrier, inc=1, device_id={'ep': mate}, device_id_type=pl.DeviceIdType.MESH)
        own_rows(0).start()
        pl.semaphore_wait(barrier, 1)
        mate_rows(0).start()
        for at in range(1, slots):
            mate_rows(at).start()
            own_rows(at).start()

    @pl.when(tile == 0)
    def _():
        for choice in range(2):
            gates = jnp.broadcast_to(gate_ref[0, choice:choice + 1, :], (LANES, tokens)).T
            keys = jnp.broadcast_to(key_ref[0, choice:choice + 1, :], (LANES, tokens)).T
            lane = lax.broadcasted_iota(jnp.int32, (block, LANES), 1)
            for half in range(2):
                src = slice(half * block, (half + 1) * block)
                rows = slice((2 * half + choice) * block, (2 * half + choice + 1) * block)
                wide_ref[rows] = gates[src]
                for col in range(0, depth, LANES):
                    pick_ref[rows, col:col + LANES] = jnp.where(keys[src] == lane + col, 1.0, 0.0).astype(pick_ref.dtype)

    @pl.when(tile % per_slot == 0)
    def _():
        own_rows(slot).wait()
        arriving = mate_rows(slot)
        arriving.wait_recv()
        arriving.wait_send()

    table = table_ref[slot, :, :, pl.ds(pl.multiple_of(tile % per_slot * width, width), width)].reshape(depth, width)
    mixed = []
    for half in range(2):
        base = 2 * half * block
        picked = jnp.dot(pick_ref[base:base + 2 * block], table, preferred_element_type=jnp.float32)
        first, second = wide_ref[base:base + block], wide_ref[base + block:base + 2 * block]
        strips = []
        for col in range(0, width, LANES):
            cols = slice(col, col + LANES)
            gated = first * picked[:block, cols] + second * picked[block:, cols]
            strips.append((res_ref[0, 0, half * block:(half + 1) * block, cols].astype(jnp.float32) + gated).astype(jnp.bfloat16))
        mixed.append(jnp.concatenate(strips, axis=1))
    for at, out_ref in enumerate(out_refs):
        @pl.when(step == at)
        def _(out_ref=out_ref):
            for half in range(2):
                out_ref[half * block:(half + 1) * block] = mixed[half]


def combine(micros, call_id, keys, gates, expert_out, residual, width):
    _, experts, capacity, d_model = expert_out.shape
    src_slots = capacity // 2
    tokens = residual.shape[2]
    depth = 2 * experts * src_slots
    count, tiles, base = len(micros), d_model // width, micros[0]
    slots = 2 * count

    def out_spec(at):
        return pl.BlockSpec((tokens, width), lambda m, n: (0, jnp.where(m < at, 0, jnp.where(m > at, tiles - 1, n))))

    return pl.pallas_call(
        functools.partial(combine_kernel, micros),
        out_shape=[jax.ShapeDtypeStruct((tokens, d_model), jnp.bfloat16)] * count,
        grid=(count, tiles),
        in_specs=[
            pl.BlockSpec((1, 2, tokens), lambda m, n: (base + m, 0, 0)),
            pl.BlockSpec((1, 2, tokens), lambda m, n: (base + m, 0, 0)),
            pl.BlockSpec(memory_space=pl.ANY),
            pl.BlockSpec((1, 1, tokens, width), lambda m, n: (base + m, 0, 0, n)),
        ],
        out_specs=[out_spec(at) for at in range(count)],
        scratch_shapes=[
            pltpu.VMEM((slots, 2 * experts, src_slots, d_model * count // slots), jnp.bfloat16),
            pltpu.VMEM((2 * tokens, depth), jnp.bfloat16),
            pltpu.VMEM((2 * tokens, LANES), jnp.float32),
            pltpu.SemaphoreType.DMA((slots,)),
            pltpu.SemaphoreType.DMA((slots,)),
            pltpu.SemaphoreType.DMA((slots,)),
        ],
        compiler_params=pltpu.CompilerParams(vmem_limit_bytes=60 << 20, collective_id=call_id, has_side_effects=True),
        cost_estimate=pl.CostEstimate(flops=4 * count * tokens * depth * d_model, bytes_accessed=2 * count * d_model * (depth + 2 * tokens), transcendentals=0),
        name='combine',
    )(keys, gates, expert_out, residual)


def regroup_kernel(wt_ref, out_ref, wide_ref):
    _, rows, width = out_ref.shape
    head_dim = wt_ref.shape[3]
    sub = wide_ref.shape[1] // rows
    per_group = width // head_dim
    for at in range(wt_ref.shape[2] // sub):
        wide = wide_ref.at[at % 2]
        wide[...] = wt_ref[0, :, at * sub:(at + 1) * sub].astype(jnp.float32).reshape(rows * sub, head_dim)
        for head in range(sub):
            group, place = divmod(at * sub + head, per_group)
            out_ref[group, :, place * head_dim:(place + 1) * head_dim] = wide[pl.ds(head, rows, stride=sub), :].astype(out_ref.dtype)


def regroup(weight, rows, width):
    _, d_model, num_heads, head_dim = weight.shape
    groups = num_heads * head_dim // width
    sub = 8
    return pl.pallas_call(
        regroup_kernel,
        out_shape=jax.ShapeDtypeStruct((groups, d_model, width), weight.dtype),
        grid=(d_model // rows,),
        in_specs=[pl.BlockSpec((1, rows, num_heads, head_dim), lambda r: (0, r, 0, 0))],
        out_specs=pl.BlockSpec((groups, rows, width), lambda r: (0, r, 0)),
        scratch_shapes=[pltpu.VMEM((2, rows * sub, head_dim), jnp.float32)],
        compiler_params=pltpu.CompilerParams(vmem_limit_bytes=60 << 20),
        cost_estimate=pl.CostEstimate(flops=10 ** 10, bytes_accessed=4 * d_model * num_heads * head_dim, transcendentals=0),
        name='regroup',
    )(weight)


def attend(q_ref, k_ref, v_ref, head, part):
    seq_len, head_dim = q_ref.shape[0], LANES
    block = seq_len // 2
    cols = slice(head * head_dim, (head + 1) * head_dim)
    rows = slice(part * block, (part + 1) * block)
    contract = (((1,), (1,)), ((), ()))
    query = q_ref[rows, cols]
    seen = lax.broadcasted_iota(jnp.int32, (block, block), 0) >= lax.broadcasted_iota(jnp.int32, (block, block), 1)
    last = lax.dot_general(query, k_ref[rows, cols], contract, preferred_element_type=jnp.float32)
    scores = jnp.where(seen, last, -jnp.inf)
    if part:
        early = lax.dot_general(query, k_ref[:block, cols], contract, preferred_element_type=jnp.float32)
        scores = jnp.concatenate([early, scores], axis=1)
    top = jnp.max(scores, axis=1, keepdims=True)
    grown = jnp.exp2((scores - top) * ((head_dim ** -0.5) * LOG2E))
    probs = (grown * (1.0 / jnp.sum(grown, axis=1, keepdims=True))).astype(jnp.bfloat16)
    mixed = jnp.dot(probs, v_ref[:(part + 1) * block, cols], preferred_element_type=jnp.float32)
    return rows, mixed.astype(jnp.bfloat16)


def attention_kernel(norm_ref, y_hbm, wq_hbm, wk_hbm, wv_hbm, wo_hbm, *refs):
    out_ref, y_ref, x_ref, attn_ref, wt_ref, wo_ref, *head_refs, y_sem, wt_sem, wo_sem = refs[-15:]
    fresh, ready = head_refs[:3], head_refs[3:]
    seq_len, d_model = y_ref.shape
    depth = attn_ref.shape[1]
    steps, _, width = wq_hbm.shape
    tile = wo_ref.shape[2]
    units = [(head, part) for head in range(width // LANES) for part in range(2)]
    step = pl.program_id(0)

    def wt_copies(at):
        return [pltpu.make_async_copy(hbm.at[at], wt_ref.at[at % 2, which], wt_sem.at[at % 2, which]) for which, hbm in enumerate((wq_hbm, wk_hbm, wv_hbm))]

    def wo_copy(at):
        cols = pl.ds(pl.multiple_of(at * tile, tile), tile)
        return pltpu.make_async_copy(wo_hbm.at[:, cols], wo_ref.at[at % 2], wo_sem.at[at % 2])

    def finish(at, proj):
        y_tile = y_ref[:, pl.ds(pl.multiple_of(at * tile, tile), tile)]
        rounded = proj.astype(jnp.bfloat16).astype(jnp.float32)
        out_ref[0, 0] = (y_tile.astype(jnp.float32) + rounded).astype(out_ref.dtype)

    @pl.when(step == 0)
    def _():
        y_copy = pltpu.make_async_copy(y_hbm, y_ref, y_sem)
        y_copy.start()
        for copy in wt_copies(0):
            copy.start()
        y_copy.wait()
        strip = 32

        def norm_strip(at, carry):
            rows = pl.ds(pl.multiple_of(at * strip, strip), strip)
            y_wide = y_ref[rows, :].astype(jnp.float32)
            inv_rms = lax.rsqrt(jnp.mean(y_wide * y_wide, axis=-1, keepdims=True) + NORM_EPS)
            x_ref[rows, :] = (y_wide * inv_rms * norm_ref[...]).astype(x_ref.dtype)
            return carry

        lax.fori_loop(0, seq_len // strip, norm_strip, 0)
        for ref in ready:
            ref[...] = jnp.zeros_like(ref)

    @pl.when(step < steps)
    def _():
        @pl.when(step < steps - 1)
        def _():
            for copy in wt_copies(step + 1):
                copy.start()

        @pl.when(step == steps - 1)
        def _():
            wo_copy(0).start()

        for copy in wt_copies(step):
            copy.wait()
        slot = step % 2
        base = jnp.where(step == 0, steps - 1, step - 1) * width
        share = (len(units) + 2) // 3
        for which in range(3):
            fresh[which][...] = jnp.dot(x_ref[...], wt_ref[slot, which], preferred_element_type=jnp.float32).astype(jnp.bfloat16)
            for head, part in units[which * share:(which + 1) * share]:
                rows, mixed = attend(*ready, head, part)
                attn_ref[rows, pl.ds(pl.multiple_of(base + head * LANES, LANES), LANES)] = mixed
        for src_ref, dst_ref in zip(fresh, ready):
            dst_ref[...] = src_ref[...]

    @pl.when(step == steps)
    def _():
        wo_copy(1).start()
        wo_copy(0).wait()
        early = depth - width
        proj = jnp.dot(attn_ref[:, :early], wo_ref[0, :early], preferred_element_type=jnp.float32)
        for head, part in units:
            rows, mixed = attend(*ready, head, part)
            attn_ref[rows, early + head * LANES:early + (head + 1) * LANES] = mixed
        finish(0, proj + jnp.dot(attn_ref[:, early:], wo_ref[0, early:], preferred_element_type=jnp.float32))

    @pl.when(step > steps)
    def _():
        at = step - steps

        @pl.when(at + 1 < d_model // tile)
        def _():
            wo_copy(at + 1).start()

        wo_copy(at).wait()
        finish(at, jnp.dot(attn_ref[...], wo_ref[at % 2], preferred_element_type=jnp.float32))


def attention(micro, arrived, norm_w, weights, w_out, result, out_shape, tile):
    seq_len, d_model = arrived.shape
    steps, _, width = weights[0].shape
    depth = steps * width
    hbm = pl.BlockSpec(memory_space=pl.ANY)
    operands = [norm_w, arrived, *weights, w_out]
    aliases = {}
    if result is not None:
        operands.append(result)
        aliases = {len(operands) - 1: 0}
    head_group = pltpu.VMEM((seq_len, width), jnp.bfloat16)
    return pl.pallas_call(
        attention_kernel,
        out_shape=jax.ShapeDtypeStruct(out_shape, jnp.bfloat16),
        grid=(steps + d_model // tile,),
        in_specs=[pl.BlockSpec((1, d_model), lambda h: (0, 0))] + [hbm] * (len(operands) - 1),
        out_specs=pl.BlockSpec((1, 1, seq_len, tile), lambda h: (micro, 0, 0, jnp.maximum(h - steps, 0))),
        scratch_shapes=[
            pltpu.VMEM((seq_len, d_model), jnp.bfloat16),
            pltpu.VMEM((seq_len, d_model), jnp.bfloat16),
            pltpu.VMEM((seq_len, depth), jnp.bfloat16),
            pltpu.VMEM((2, 3, d_model, width), jnp.bfloat16),
            pltpu.VMEM((2, depth, tile), jnp.bfloat16),
            *[head_group] * 6,
            pltpu.SemaphoreType.DMA,
            pltpu.SemaphoreType.DMA((2, 3)),
            pltpu.SemaphoreType.DMA((2,)),
        ],
        input_output_aliases=aliases,
        compiler_params=pltpu.CompilerParams(vmem_limit_bytes=60 << 20),
        cost_estimate=pl.CostEstimate(flops=8 * seq_len * d_model * depth, bytes_accessed=8 * d_model * depth, transcendentals=0),
        name='attention',
    )(*operands)


def solution(mesh):
    stages = mesh.shape['pp']
    group_size = mesh.shape['ep']
    send_next = [(src, (src + 1) % stages) for src in range(stages)]
    tok_spec = P('pp', 'ep', None, None)
    wt_spec = P('pp', None, None, None)

    def device_step(expert_out, expert_ids, slot_ids, gate_vals, residual, norm_w, w_query, w_key, w_value, w_out):
        num_micro, _, _, d_model = residual.shape
        experts, capacity = expert_out.shape[1:3]
        src_slots = capacity // group_size
        num_experts = experts * group_size
        position = lax.axis_index('ep').astype(jnp.int32)

        place = (expert_ids[:, 0] - position * experts) % num_experts
        keys = jnp.where(slot_ids[:, 0] >= 0, place * src_slots + slot_ids[:, 0] - position * src_slots, -1)
        keys = jnp.swapaxes(keys, 1, 2)
        gates = jnp.swapaxes(gate_vals[:, 0], 1, 2)

        arrived = []
        combined = []
        for call_id, micros in enumerate(((0,), (1, 2), (3, 4, 5))):
            if combined:
                keys = lax.optimization_barrier((keys, combined[-1]))[0]
            rows = combine(micros, call_id, keys, gates, expert_out, residual, 512)
            combined.extend(rows)
            for micro, row in zip(micros, rows):
                arrived.append(lax.ppermute(row, 'pp', send_next))
        raw = lax.optimization_barrier((w_query, w_key, w_value, combined[-1]))[:3]
        weights = [regroup(wt, 256, 512) for wt in raw]

        flat_out = w_out[0].reshape(-1, d_model)
        result = None
        for micro in range(num_micro):
            rows = arrived[micro]
            if micro:
                rows, result = lax.optimization_barrier((rows, result))
            result = attention(micro, rows, norm_w, weights, flat_out, result, residual.shape, 512)
        return result

    return jax.shard_map(device_step, mesh=mesh, in_specs=(tok_spec, tok_spec, tok_spec, tok_spec, tok_spec, P('pp', None), wt_spec, wt_spec, wt_spec, wt_spec), out_specs=tok_spec, check_vma=False)
```

```python
import functools

import jax
import jax.numpy as jnp
from jax import lax
from jax.experimental import pallas as pl
from jax.experimental.pallas import tpu as pltpu
from jax.sharding import PartitionSpec as P


NORM_EPS = 1e-6
LOG2E = 1.4426950408889634
LANES = 128


def combine_kernel(micros, key_ref, gate_ref, expert_ref, res_ref, *refs):
    count = len(micros)
    out_refs = refs[:count]
    table_ref, pick_ref, wide_ref, own_sem, send_sem, recv_sem = refs[count:]
    slots = table_ref.shape[0]
    experts, src_slots, span = table_ref.shape[1] // 2, table_ref.shape[2], table_ref.shape[3]
    halves, tokens, width = slots // count, out_refs[0].shape[0], out_refs[0].shape[1]
    per_slot = span // width
    depth = pick_ref.shape[1]
    block = tokens // 2
    step, tile = pl.program_id(0), pl.program_id(1)
    slot = step * halves + tile // per_slot
    me = lax.axis_index('ep')
    mate = 1 - me

    def own_rows(slot):
        cols = pl.ds(pl.multiple_of(slot % halves * span, span), span)
        rows = pl.ds(pl.multiple_of(me * src_slots, src_slots), src_slots)
        return pltpu.make_async_copy(expert_ref.at[micros[0] + slot // halves, :, rows, cols], table_ref.at[slot, :experts], own_sem.at[slot])

    def mate_rows(slot):
        cols = pl.ds(pl.multiple_of(slot % halves * span, span), span)
        rows = pl.ds(pl.multiple_of(mate * src_slots, src_slots), src_slots)
        return pltpu.make_async_remote_copy(
            src_ref=expert_ref.at[micros[0] + slot // halves, :, rows, cols],
            dst_ref=table_ref.at[slot, experts:],
            send_sem=send_sem.at[slot],
            recv_sem=recv_sem.at[slot],
            device_id={'ep': mate},
            device_id_type=pl.DeviceIdType.MESH,
        )

    @pl.when((step == 0) & (tile == 0))
    def _():
        barrier = pltpu.get_barrier_semaphore()
        pl.semaphore_signal(barrier, inc=1, device_id={'ep': mate}, device_id_type=pl.DeviceIdType.MESH)
        own_rows(0).start()
        pl.semaphore_wait(barrier, 1)
        mate_rows(0).start()
        for at in range(1, slots):
            mate_rows(at).start()
            own_rows(at).start()

    @pl.when(tile == 0)
    def _():
        for choice in range(2):
            gates = jnp.broadcast_to(gate_ref[0, choice:choice + 1, :], (LANES, tokens)).T
            keys = jnp.broadcast_to(key_ref[0, choice:choice + 1, :], (LANES, tokens)).T
            lane = lax.broadcasted_iota(jnp.int32, (block, LANES), 1)
            for half in range(2):
                src = slice(half * block, (half + 1) * block)
                rows = slice((2 * half + choice) * block, (2 * half + choice + 1) * block)
                wide_ref[rows] = gates[src]
                for col in range(0, depth, LANES):
                    pick_ref[rows, col:col + LANES] = jnp.where(keys[src] == lane + col, 1.0, 0.0).astype(pick_ref.dtype)

    @pl.when(tile % per_slot == 0)
    def _():
        own_rows(slot).wait()
        arriving = mate_rows(slot)
        arriving.wait_recv()
        arriving.wait_send()

    table = table_ref[slot, :, :, pl.ds(pl.multiple_of(tile % per_slot * width, width), width)].reshape(depth, width)
    mixed = []
    for half in range(2):
        base = 2 * half * block
        picked = jnp.dot(pick_ref[base:base + 2 * block], table, preferred_element_type=jnp.float32)
        first, second = wide_ref[base:base + block], wide_ref[base + block:base + 2 * block]
        strips = []
        for col in range(0, width, LANES):
            cols = slice(col, col + LANES)
            gated = first * picked[:block, cols] + second * picked[block:, cols]
            strips.append((res_ref[0, 0, half * block:(half + 1) * block, cols].astype(jnp.float32) + gated).astype(jnp.bfloat16))
        mixed.append(jnp.concatenate(strips, axis=1))
    for at, out_ref in enumerate(out_refs):
        @pl.when(step == at)
        def _(out_ref=out_ref):
            for half in range(2):
                out_ref[half * block:(half + 1) * block] = mixed[half]


def combine(micros, call_id, keys, gates, expert_out, residual, width):
    _, experts, capacity, d_model = expert_out.shape
    src_slots = capacity // 2
    tokens = residual.shape[2]
    depth = 2 * experts * src_slots
    count, tiles, base = len(micros), d_model // width, micros[0]
    slots = tiles * count

    def out_spec(at):
        return pl.BlockSpec((tokens, width), lambda m, n: (0, jnp.where(m < at, 0, jnp.where(m > at, tiles - 1, n))))

    return pl.pallas_call(
        functools.partial(combine_kernel, micros),
        out_shape=[jax.ShapeDtypeStruct((tokens, d_model), jnp.bfloat16)] * count,
        grid=(count, tiles),
        in_specs=[
            pl.BlockSpec((1, 2, tokens), lambda m, n: (base + m, 0, 0)),
            pl.BlockSpec((1, 2, tokens), lambda m, n: (base + m, 0, 0)),
            pl.BlockSpec(memory_space=pl.ANY),
            pl.BlockSpec((1, 1, tokens, width), lambda m, n: (base + m, 0, 0, n)),
        ],
        out_specs=[out_spec(at) for at in range(count)],
        scratch_shapes=[
            pltpu.VMEM((slots, 2 * experts, src_slots, d_model * count // slots), jnp.bfloat16),
            pltpu.VMEM((2 * tokens, depth), jnp.bfloat16),
            pltpu.VMEM((2 * tokens, LANES), jnp.float32),
            pltpu.SemaphoreType.DMA((slots,)),
            pltpu.SemaphoreType.DMA((slots,)),
            pltpu.SemaphoreType.DMA((slots,)),
        ],
        compiler_params=pltpu.CompilerParams(vmem_limit_bytes=60 << 20, collective_id=call_id, has_side_effects=True),
        cost_estimate=pl.CostEstimate(flops=4 * count * tokens * depth * d_model, bytes_accessed=2 * count * d_model * (depth + 2 * tokens), transcendentals=0),
        name='combine',
    )(keys, gates, expert_out, residual)


def regroup_kernel(wt_ref, out_ref, wide_ref):
    _, rows, width = out_ref.shape
    head_dim = wt_ref.shape[3]
    sub = wide_ref.shape[1] // rows
    per_group = width // head_dim
    for at in range(wt_ref.shape[2] // sub):
        wide = wide_ref.at[at % 2]
        wide[...] = wt_ref[0, :, at * sub:(at + 1) * sub].astype(jnp.float32).reshape(rows * sub, head_dim)
        for head in range(sub):
            group, place = divmod(at * sub + head, per_group)
            out_ref[group, :, place * head_dim:(place + 1) * head_dim] = wide[pl.ds(head, rows, stride=sub), :].astype(out_ref.dtype)


def regroup(position, weight, rows, width):
    _, d_model, num_heads, head_dim = weight.shape
    heads = num_heads // 2
    groups = heads * head_dim // width
    sub = 8
    return pl.pallas_call(
        lambda pos_ref, *refs: regroup_kernel(*refs),
        out_shape=jax.ShapeDtypeStruct((groups, d_model, width), weight.dtype),
        grid_spec=pltpu.PrefetchScalarGridSpec(
            num_scalar_prefetch=1,
            grid=(d_model // rows,),
            in_specs=[pl.BlockSpec((1, rows, heads, head_dim), lambda r, pos: (0, r, pos[0], 0))],
            out_specs=pl.BlockSpec((groups, rows, width), lambda r, pos: (0, r, 0)),
            scratch_shapes=[pltpu.VMEM((2, rows * sub, head_dim), jnp.float32)],
        ),
        compiler_params=pltpu.CompilerParams(vmem_limit_bytes=60 << 20),
        cost_estimate=pl.CostEstimate(flops=10 ** 10, bytes_accessed=2 * d_model * num_heads * head_dim, transcendentals=0),
        name='regroup',
    )(position, weight)


def score(q_ref, k_ref, score_ref, head, part):
    block = q_ref.shape[0] // 2
    cols = slice(head * LANES, (head + 1) * LANES)
    keys = (part + 1) * block
    score_ref[:, :keys] = lax.dot_general(q_ref[part * block:keys, cols], k_ref[:keys, cols], (((1,), (1,)), ((), ())), preferred_element_type=jnp.float32)


def causal_softmax(score_ref, prob_ref, part):
    block = score_ref.shape[0]
    strip = 32
    keys = (part + 1) * block
    row_pos = lax.broadcasted_iota(jnp.int32, (strip, LANES), 0)
    col_pos = lax.broadcasted_iota(jnp.int32, (strip, LANES), 1)
    for at in range(0, block, strip):
        here = slice(at, at + strip)
        diagonal = (part * block + at) // LANES * LANES
        seen = row_pos + (part * block + at - diagonal) >= col_pos
        last = jnp.where(seen, score_ref[here, diagonal:diagonal + LANES], -jnp.inf)
        pieces = [score_ref[here, col:col + LANES] for col in range(0, diagonal, LANES)] + [last]
        top = jnp.max(functools.reduce(jnp.maximum, pieces), axis=1, keepdims=True)
        pieces = [jnp.exp2((piece - top) * ((LANES ** -0.5) * LOG2E)) for piece in pieces]
        scale = 1.0 / jnp.sum(functools.reduce(jnp.add, pieces), axis=1, keepdims=True)
        for which, piece in enumerate(pieces):
            prob_ref[here, which * LANES:(which + 1) * LANES] = (piece * scale).astype(jnp.bfloat16)
        if diagonal + LANES < keys:
            prob_ref[here, diagonal + LANES:keys] = jnp.zeros((strip, keys - diagonal - LANES), jnp.bfloat16)


def attention_kernel(norm_ref, y_hbm, wq_hbm, wk_hbm, wv_hbm, oq_hbm, ok_hbm, ov_hbm, wo_hbm, *refs):
    out_ref, y_ref, x_ref, attn_ref, wt_ref, wo_ref, q_ref, k_ref, v_ref, *unit_refs, y_sem, wt_sem, wo_sem = refs[-28:]
    score_refs, prob_refs = unit_refs[:8], unit_refs[8:]
    seq_len, d_model = y_ref.shape
    own_groups, _, width = wq_hbm.shape
    steps = 2 * own_groups
    tile = wo_ref.shape[2]
    step = pl.program_id(0)
    me = lax.axis_index('ep')

    def wt_copies(at, sources):
        return [pltpu.make_async_copy(hbm.at[at % own_groups], wt_ref.at[at % 2, which], wt_sem.at[at % 2, which]) for which, hbm in enumerate(sources)]

    def start_weights(at):
        @pl.when(at // own_groups == me)
        def _():
            for copy in wt_copies(at, (wq_hbm, wk_hbm, wv_hbm)):
                copy.start()

        @pl.when(at // own_groups != me)
        def _():
            for copy in wt_copies(at, (oq_hbm, ok_hbm, ov_hbm)):
                copy.start()

    def wo_copy(at):
        cols = pl.ds(pl.multiple_of(at * tile, tile), tile)
        return pltpu.make_async_copy(wo_hbm.at[:, cols], wo_ref.at[at % 2], wo_sem.at[at % 2])

    @pl.when(step == 0)
    def _():
        y_copy = pltpu.make_async_copy(y_hbm, y_ref, y_sem)
        y_copy.start()
        start_weights(step)
        y_copy.wait()
        strip = 32

        def norm_strip(at, carry):
            rows = pl.ds(pl.multiple_of(at * strip, strip), strip)
            y_wide = y_ref[rows, :].astype(jnp.float32)
            inv_rms = lax.rsqrt(jnp.mean(y_wide * y_wide, axis=-1, keepdims=True) + NORM_EPS)
            x_ref[rows, :] = (y_wide * inv_rms * norm_ref[...]).astype(x_ref.dtype)
            return carry

        lax.fori_loop(0, seq_len // strip, norm_strip, 0)

    @pl.when(step < steps)
    def _():
        @pl.when(step < steps - 1)
        def _():
            start_weights(step + 1)

        @pl.when(step == steps - 1)
        def _():
            wo_copy(0).start()

        for copy in wt_copies(step, (wq_hbm, wk_hbm, wv_hbm)):
            copy.wait()
        slot = step % 2

        def emit(which, dst_ref):
            dst_ref[...] = jnp.dot(x_ref[...], wt_ref[slot, which], preferred_element_type=jnp.float32).astype(jnp.bfloat16)

        block = seq_len // 2
        units = [(head, part) for head in range(width // LANES) for part in range(2)]
        emit(0, q_ref)
        emit(1, k_ref)
        for at, (head, part) in enumerate(units):
            score(q_ref, k_ref, score_refs[at], head, part)
        emit(2, v_ref)
        for at, (head, part) in enumerate(units):
            causal_softmax(score_refs[at], prob_refs[at], part)
        for at, (head, part) in enumerate(units):
            keys = (part + 1) * block
            mixed = jnp.dot(prob_refs[at][:, :keys], v_ref[:keys, head * LANES:(head + 1) * LANES], preferred_element_type=jnp.float32)
            attn_ref[part * block:keys, pl.ds(pl.multiple_of(step * width + head * LANES, LANES), LANES)] = mixed.astype(jnp.bfloat16)

    @pl.when(step >= steps)
    def _():
        at = step - steps

        @pl.when(at + 1 < d_model // tile)
        def _():
            wo_copy(at + 1).start()

        wo_copy(at).wait()
        proj = jnp.dot(attn_ref[...], wo_ref[at % 2], preferred_element_type=jnp.float32).astype(jnp.bfloat16)
        y_tile = y_ref[:, pl.ds(pl.multiple_of(at * tile, tile), tile)]
        out_ref[0, 0] = (y_tile.astype(jnp.float32) + proj.astype(jnp.float32)).astype(out_ref.dtype)


def attention(micro, arrived, norm_w, weights, w_out, result, out_shape, tile):
    seq_len, d_model = arrived.shape
    steps, _, width = weights[0].shape
    steps = 2 * steps
    depth = steps * width
    hbm = pl.BlockSpec(memory_space=pl.ANY)
    operands = [norm_w, arrived, *weights, w_out]
    aliases = {}
    if result is not None:
        operands.append(result)
        aliases = {len(operands) - 1: 0}
    head_group = pltpu.VMEM((seq_len, width), jnp.bfloat16)
    return pl.pallas_call(
        attention_kernel,
        out_shape=jax.ShapeDtypeStruct(out_shape, jnp.bfloat16),
        grid=(steps + d_model // tile,),
        in_specs=[pl.BlockSpec((1, d_model), lambda h: (0, 0))] + [hbm] * (len(operands) - 1),
        out_specs=pl.BlockSpec((1, 1, seq_len, tile), lambda h: (micro, 0, 0, jnp.maximum(h - steps, 0))),
        scratch_shapes=[
            pltpu.VMEM((seq_len, d_model), jnp.bfloat16),
            pltpu.VMEM((seq_len, d_model), jnp.bfloat16),
            pltpu.VMEM((seq_len, depth), jnp.bfloat16),
            pltpu.VMEM((2, 3, d_model, width), jnp.bfloat16),
            pltpu.VMEM((2, depth, tile), jnp.bfloat16),
            *[head_group] * 3,
            *[pltpu.VMEM((seq_len // 2, seq_len), jnp.float32)] * 8,
            *[pltpu.VMEM((seq_len // 2, seq_len), jnp.bfloat16)] * 8,
            pltpu.SemaphoreType.DMA,
            pltpu.SemaphoreType.DMA((2, 3)),
            pltpu.SemaphoreType.DMA((2,)),
        ],
        input_output_aliases=aliases,
        compiler_params=pltpu.CompilerParams(vmem_limit_bytes=60 << 20),
        cost_estimate=pl.CostEstimate(flops=8 * seq_len * d_model * depth, bytes_accessed=8 * d_model * depth, transcendentals=0),
        name='attention',
    )(*operands)


def solution(mesh):
    stages = mesh.shape['pp']
    group_size = mesh.shape['ep']
    send_next = [(src, (src + 1) % stages) for src in range(stages)]
    swap_pair = [(src, (src + 1) % group_size) for src in range(group_size)]
    tok_spec = P('pp', 'ep', None, None)
    wt_spec = P('pp', None, None, None)

    def device_step(expert_out, expert_ids, slot_ids, gate_vals, residual, norm_w, w_query, w_key, w_value, w_out):
        num_micro, _, _, d_model = residual.shape
        experts, capacity = expert_out.shape[1:3]
        src_slots = capacity // group_size
        num_experts = experts * group_size
        position = lax.axis_index('ep').astype(jnp.int32)

        place = (expert_ids[:, 0] - position * experts) % num_experts
        keys = jnp.where(slot_ids[:, 0] >= 0, place * src_slots + slot_ids[:, 0] - position * src_slots, -1)
        keys = jnp.swapaxes(keys, 1, 2)
        gates = jnp.swapaxes(gate_vals[:, 0], 1, 2)

        halves = []
        for wt in (w_query, w_key, w_value):
            if halves:
                wt = lax.optimization_barrier((wt, halves[-1]))[0]
            halves.append(regroup(position[None], wt, 256, 512))
        crossed = []
        for half in halves:
            crossed.append(lax.ppermute(half, 'ep', swap_pair))
        weights = [*halves, *crossed]

        keys = lax.optimization_barrier((keys, halves[-1]))[0]
        arrived = []
        combined = []
        for call_id, micros in enumerate(((0,), (1, 2), (3, 4, 5))):
            if combined:
                keys = lax.optimization_barrier((keys, combined[-1]))[0]
            rows = combine(micros, call_id, keys, gates, expert_out, residual, 512)
            combined.extend(rows)
            for micro, row in zip(micros, rows):
                arrived.append(lax.ppermute(row, 'pp', send_next))

        flat_out = w_out[0].reshape(-1, d_model)
        result = None
        for micro in range(num_micro):
            rows = lax.optimization_barrier((arrived[0], combined[-1]))[0] if micro == 0 else arrived[micro]
            if micro:
                rows, result = lax.optimization_barrier((rows, result))
            result = attention(micro, rows, norm_w, weights, flat_out, result, residual.shape, 512)
        return result

    return jax.shard_map(device_step, mesh=mesh, in_specs=(tok_spec, tok_spec, tok_spec, tok_spec, tok_spec, P('pp', None), wt_spec, wt_spec, wt_spec, wt_spec), out_specs=tok_spec, check_vma=False)
```

```python
import functools

import jax
import jax.numpy as jnp
from jax import lax
from jax.experimental import pallas as pl
from jax.experimental.pallas import tpu as pltpu
from jax.sharding import PartitionSpec as P


NORM_EPS = 1e-6
LOG2E = 1.4426950408889634
LANES = 128


def combine_kernel(micros, key_ref, gate_ref, expert_ref, res_ref, *refs):
    count = len(micros)
    out_refs = refs[:count]
    table_ref, pick_ref, wide_ref, own_sem, send_sem, recv_sem = refs[count:]
    slots = table_ref.shape[0]
    experts, src_slots, span = table_ref.shape[1] // 2, table_ref.shape[2], table_ref.shape[3]
    halves, tokens, width = slots // count, out_refs[0].shape[0], out_refs[0].shape[1]
    per_slot = span // width
    depth = pick_ref.shape[1]
    block = tokens // 2
    step, tile = pl.program_id(0), pl.program_id(1)
    slot = step * halves + tile // per_slot
    me = lax.axis_index('ep')
    mate = 1 - me

    def own_rows(slot):
        cols = pl.ds(pl.multiple_of(slot % halves * span, span), span)
        rows = pl.ds(pl.multiple_of(me * src_slots, src_slots), src_slots)
        return pltpu.make_async_copy(expert_ref.at[micros[0] + slot // halves, :, rows, cols], table_ref.at[slot, :experts], own_sem.at[slot])

    def mate_rows(slot):
        cols = pl.ds(pl.multiple_of(slot % halves * span, span), span)
        rows = pl.ds(pl.multiple_of(mate * src_slots, src_slots), src_slots)
        return pltpu.make_async_remote_copy(
            src_ref=expert_ref.at[micros[0] + slot // halves, :, rows, cols],
            dst_ref=table_ref.at[slot, experts:],
            send_sem=send_sem.at[slot],
            recv_sem=recv_sem.at[slot],
            device_id={'ep': mate},
            device_id_type=pl.DeviceIdType.MESH,
        )

    @pl.when((step == 0) & (tile == 0))
    def _():
        barrier = pltpu.get_barrier_semaphore()
        pl.semaphore_signal(barrier, inc=1, device_id={'ep': mate}, device_id_type=pl.DeviceIdType.MESH)
        own_rows(0).start()
        pl.semaphore_wait(barrier, 1)
        mate_rows(0).start()
        for at in range(1, slots):
            mate_rows(at).start()
            own_rows(at).start()

    @pl.when(tile == 0)
    def _():
        for choice in range(2):
            gates = jnp.broadcast_to(gate_ref[0, choice:choice + 1, :], (LANES, tokens)).T
            keys = jnp.broadcast_to(key_ref[0, choice:choice + 1, :], (LANES, tokens)).T
            lane = lax.broadcasted_iota(jnp.int32, (block, LANES), 1)
            for half in range(2):
                src = slice(half * block, (half + 1) * block)
                rows = slice((2 * half + choice) * block, (2 * half + choice + 1) * block)
                wide_ref[rows] = gates[src]
                for col in range(0, depth, LANES):
                    pick_ref[rows, col:col + LANES] = jnp.where(keys[src] == lane + col, 1.0, 0.0).astype(pick_ref.dtype)

    @pl.when(tile % per_slot == 0)
    def _():
        own_rows(slot).wait()
        arriving = mate_rows(slot)
        arriving.wait_recv()
        arriving.wait_send()

    table = table_ref[slot, :, :, pl.ds(pl.multiple_of(tile % per_slot * width, width), width)].reshape(depth, width)
    mixed = []
    for half in range(2):
        base = 2 * half * block
        picked = jnp.dot(pick_ref[base:base + 2 * block], table, preferred_element_type=jnp.float32)
        first, second = wide_ref[base:base + block], wide_ref[base + block:base + 2 * block]
        strips = []
        for col in range(0, width, LANES):
            cols = slice(col, col + LANES)
            gated = first * picked[:block, cols] + second * picked[block:, cols]
            strips.append((res_ref[0, 0, half * block:(half + 1) * block, cols].astype(jnp.float32) + gated).astype(jnp.bfloat16))
        mixed.append(jnp.concatenate(strips, axis=1))
    for at, out_ref in enumerate(out_refs):
        @pl.when(step == at)
        def _(out_ref=out_ref):
            for half in range(2):
                out_ref[half * block:(half + 1) * block] = mixed[half]


def combine(micros, call_id, keys, gates, expert_out, residual, width):
    _, experts, capacity, d_model = expert_out.shape
    src_slots = capacity // 2
    tokens = residual.shape[2]
    depth = 2 * experts * src_slots
    count, tiles, base = len(micros), d_model // width, micros[0]
    slots = tiles * count

    def out_spec(at):
        return pl.BlockSpec((tokens, width), lambda m, n: (0, jnp.where(m < at, 0, jnp.where(m > at, tiles - 1, n))))

    return pl.pallas_call(
        functools.partial(combine_kernel, micros),
        out_shape=[jax.ShapeDtypeStruct((tokens, d_model), jnp.bfloat16)] * count,
        grid=(count, tiles),
        in_specs=[
            pl.BlockSpec((1, 2, tokens), lambda m, n: (base + m, 0, 0)),
            pl.BlockSpec((1, 2, tokens), lambda m, n: (base + m, 0, 0)),
            pl.BlockSpec(memory_space=pl.ANY),
            pl.BlockSpec((1, 1, tokens, width), lambda m, n: (base + m, 0, 0, n)),
        ],
        out_specs=[out_spec(at) for at in range(count)],
        scratch_shapes=[
            pltpu.VMEM((slots, 2 * experts, src_slots, d_model * count // slots), jnp.bfloat16),
            pltpu.VMEM((2 * tokens, depth), jnp.bfloat16),
            pltpu.VMEM((2 * tokens, LANES), jnp.float32),
            pltpu.SemaphoreType.DMA((slots,)),
            pltpu.SemaphoreType.DMA((slots,)),
            pltpu.SemaphoreType.DMA((slots,)),
        ],
        compiler_params=pltpu.CompilerParams(vmem_limit_bytes=60 << 20, collective_id=call_id, has_side_effects=True),
        cost_estimate=pl.CostEstimate(flops=4 * count * tokens * depth * d_model, bytes_accessed=2 * count * d_model * (depth + 2 * tokens), transcendentals=0),
        name='combine',
    )(keys, gates, expert_out, residual)


def regroup_kernel(wt_ref, out_ref, wide_ref):
    _, rows, width = out_ref.shape
    head_dim = wt_ref.shape[3]
    sub = wide_ref.shape[1] // rows
    per_group = width // head_dim
    for at in range(wt_ref.shape[2] // sub):
        wide = wide_ref.at[at % 2]
        wide[...] = wt_ref[0, :, at * sub:(at + 1) * sub].astype(jnp.float32).reshape(rows * sub, head_dim)
        for head in range(sub):
            group, place = divmod(at * sub + head, per_group)
            out_ref[group, :, place * head_dim:(place + 1) * head_dim] = wide[pl.ds(head, rows, stride=sub), :].astype(out_ref.dtype)


def regroup(position, weight, rows, width):
    _, d_model, num_heads, head_dim = weight.shape
    heads = num_heads // 2
    if position is None:
        heads, position = num_heads, jnp.zeros((1,), jnp.int32)
    groups = heads * head_dim // width
    sub = 8
    return pl.pallas_call(
        lambda pos_ref, *refs: regroup_kernel(*refs),
        out_shape=jax.ShapeDtypeStruct((groups, d_model, width), weight.dtype),
        grid_spec=pltpu.PrefetchScalarGridSpec(
            num_scalar_prefetch=1,
            grid=(d_model // rows,),
            in_specs=[pl.BlockSpec((1, rows, heads, head_dim), lambda r, pos: (0, r, pos[0], 0))],
            out_specs=pl.BlockSpec((groups, rows, width), lambda r, pos: (0, r, 0)),
            scratch_shapes=[pltpu.VMEM((2, rows * sub, head_dim), jnp.float32)],
        ),
        compiler_params=pltpu.CompilerParams(vmem_limit_bytes=60 << 20),
        cost_estimate=pl.CostEstimate(flops=10 ** 10, bytes_accessed=2 * d_model * num_heads * head_dim, transcendentals=0),
        name='regroup',
    )(position, weight)


def score(q_ref, k_ref, score_ref, head, part):
    block = q_ref.shape[0] // 2
    cols = slice(head * LANES, (head + 1) * LANES)
    keys = (part + 1) * block
    score_ref[:, :keys] = lax.dot_general(q_ref[part * block:keys, cols], k_ref[:keys, cols], (((1,), (1,)), ((), ())), preferred_element_type=jnp.float32)


def causal_softmax(score_ref, prob_ref, part):
    block = score_ref.shape[0]
    strip = 32
    keys = (part + 1) * block
    row_pos = lax.broadcasted_iota(jnp.int32, (strip, LANES), 0)
    col_pos = lax.broadcasted_iota(jnp.int32, (strip, LANES), 1)
    for at in range(0, block, strip):
        here = slice(at, at + strip)
        diagonal = (part * block + at) // LANES * LANES
        seen = row_pos + (part * block + at - diagonal) >= col_pos
        last = jnp.where(seen, score_ref[here, diagonal:diagonal + LANES], -jnp.inf)
        pieces = [score_ref[here, col:col + LANES] for col in range(0, diagonal, LANES)] + [last]
        top = jnp.max(functools.reduce(jnp.maximum, pieces), axis=1, keepdims=True)
        pieces = [jnp.exp2((piece - top) * ((LANES ** -0.5) * LOG2E)) for piece in pieces]
        scale = 1.0 / jnp.sum(functools.reduce(jnp.add, pieces), axis=1, keepdims=True)
        for which, piece in enumerate(pieces):
            prob_ref[here, which * LANES:(which + 1) * LANES] = (piece * scale).astype(jnp.bfloat16)
        if diagonal + LANES < keys:
            prob_ref[here, diagonal + LANES:keys] = jnp.zeros((strip, keys - diagonal - LANES), jnp.bfloat16)


def attention_kernel(norm_ref, y_hbm, wq_hbm, wk_hbm, oq_hbm, ok_hbm, wv_hbm, wo_hbm, *refs):
    out_ref, y_ref, x_ref, attn_ref, wt_ref, wo_ref, q_ref, k_ref, v_ref, *unit_refs, y_sem, wt_sem, wo_sem = refs[-28:]
    score_refs, prob_refs = unit_refs[:8], unit_refs[8:]
    seq_len, d_model = y_ref.shape
    own_groups, _, width = wq_hbm.shape
    steps = 2 * own_groups
    tile = wo_ref.shape[2]
    step = pl.program_id(0)
    me = lax.axis_index('ep')

    def wt_copies(at, query_hbm, key_hbm):
        sources = (query_hbm.at[at % own_groups], key_hbm.at[at % own_groups], wv_hbm.at[at])
        return [pltpu.make_async_copy(src, wt_ref.at[at % 2, which], wt_sem.at[at % 2, which]) for which, src in enumerate(sources)]

    def start_weights(at):
        @pl.when(at // own_groups == me)
        def _():
            for copy in wt_copies(at, wq_hbm, wk_hbm):
                copy.start()

        @pl.when(at // own_groups != me)
        def _():
            for copy in wt_copies(at, oq_hbm, ok_hbm):
                copy.start()

    def wo_copy(at):
        cols = pl.ds(pl.multiple_of(at * tile, tile), tile)
        return pltpu.make_async_copy(wo_hbm.at[:, cols], wo_ref.at[at % 2], wo_sem.at[at % 2])

    @pl.when(step == 0)
    def _():
        y_copy = pltpu.make_async_copy(y_hbm, y_ref, y_sem)
        y_copy.start()
        start_weights(step)
        y_copy.wait()
        strip = 32

        def norm_strip(at, carry):
            rows = pl.ds(pl.multiple_of(at * strip, strip), strip)
            y_wide = y_ref[rows, :].astype(jnp.float32)
            inv_rms = lax.rsqrt(jnp.mean(y_wide * y_wide, axis=-1, keepdims=True) + NORM_EPS)
            x_ref[rows, :] = (y_wide * inv_rms * norm_ref[...]).astype(x_ref.dtype)
            return carry

        lax.fori_loop(0, seq_len // strip, norm_strip, 0)

    @pl.when(step < steps)
    def _():
        @pl.when(step < steps - 1)
        def _():
            start_weights(step + 1)

        @pl.when(step == steps - 1)
        def _():
            wo_copy(0).start()

        for copy in wt_copies(step, wq_hbm, wk_hbm):
            copy.wait()
        slot = step % 2

        def emit(which, dst_ref):
            dst_ref[...] = jnp.dot(x_ref[...], wt_ref[slot, which], preferred_element_type=jnp.float32).astype(jnp.bfloat16)

        block = seq_len // 2
        units = [(head, part) for head in range(width // LANES) for part in range(2)]
        emit(0, q_ref)
        emit(1, k_ref)
        for at, (head, part) in enumerate(units):
            score(q_ref, k_ref, score_refs[at], head, part)
        emit(2, v_ref)
        for at, (head, part) in enumerate(units):
            causal_softmax(score_refs[at], prob_refs[at], part)
        for at, (head, part) in enumerate(units):
            keys = (part + 1) * block
            mixed = jnp.dot(prob_refs[at][:, :keys], v_ref[:keys, head * LANES:(head + 1) * LANES], preferred_element_type=jnp.float32)
            attn_ref[part * block:keys, pl.ds(pl.multiple_of(step * width + head * LANES, LANES), LANES)] = mixed.astype(jnp.bfloat16)

    @pl.when(step >= steps)
    def _():
        at = step - steps

        @pl.when(at + 1 < d_model // tile)
        def _():
            wo_copy(at + 1).start()

        wo_copy(at).wait()
        proj = jnp.dot(attn_ref[...], wo_ref[at % 2], preferred_element_type=jnp.float32).astype(jnp.bfloat16)
        y_tile = y_ref[:, pl.ds(pl.multiple_of(at * tile, tile), tile)]
        out_ref[0, 0] = (y_tile.astype(jnp.float32) + proj.astype(jnp.float32)).astype(out_ref.dtype)


def attention(micro, arrived, norm_w, weights, w_out, result, out_shape, tile):
    seq_len, d_model = arrived.shape
    steps, _, width = weights[0].shape
    steps = 2 * steps
    depth = steps * width
    hbm = pl.BlockSpec(memory_space=pl.ANY)
    operands = [norm_w, arrived, *weights, w_out]
    aliases = {}
    if result is not None:
        operands.append(result)
        aliases = {len(operands) - 1: 0}
    head_group = pltpu.VMEM((seq_len, width), jnp.bfloat16)
    return pl.pallas_call(
        attention_kernel,
        out_shape=jax.ShapeDtypeStruct(out_shape, jnp.bfloat16),
        grid=(steps + d_model // tile,),
        in_specs=[pl.BlockSpec((1, d_model), lambda h: (0, 0))] + [hbm] * (len(operands) - 1),
        out_specs=pl.BlockSpec((1, 1, seq_len, tile), lambda h: (micro, 0, 0, jnp.maximum(h - steps, 0))),
        scratch_shapes=[
            pltpu.VMEM((seq_len, d_model), jnp.bfloat16),
            pltpu.VMEM((seq_len, d_model), jnp.bfloat16),
            pltpu.VMEM((seq_len, depth), jnp.bfloat16),
            pltpu.VMEM((2, 3, d_model, width), jnp.bfloat16),
            pltpu.VMEM((2, depth, tile), jnp.bfloat16),
            *[head_group] * 3,
            *[pltpu.VMEM((seq_len // 2, seq_len), jnp.float32)] * 8,
            *[pltpu.VMEM((seq_len // 2, seq_len), jnp.bfloat16)] * 8,
            pltpu.SemaphoreType.DMA,
            pltpu.SemaphoreType.DMA((2, 3)),
            pltpu.SemaphoreType.DMA((2,)),
        ],
        input_output_aliases=aliases,
        compiler_params=pltpu.CompilerParams(vmem_limit_bytes=60 << 20),
        cost_estimate=pl.CostEstimate(flops=8 * seq_len * d_model * depth, bytes_accessed=8 * d_model * depth, transcendentals=0),
        name='attention',
    )(*operands)


def solution(mesh):
    stages = mesh.shape['pp']
    group_size = mesh.shape['ep']
    send_next = [(src, (src + 1) % stages) for src in range(stages)]
    swap_pair = [(src, (src + 1) % group_size) for src in range(group_size)]
    tok_spec = P('pp', 'ep', None, None)
    wt_spec = P('pp', None, None, None)

    def device_step(expert_out, expert_ids, slot_ids, gate_vals, residual, norm_w, w_query, w_key, w_value, w_out):
        num_micro, _, _, d_model = residual.shape
        experts, capacity = expert_out.shape[1:3]
        src_slots = capacity // group_size
        num_experts = experts * group_size
        position = lax.axis_index('ep').astype(jnp.int32)

        place = (expert_ids[:, 0] - position * experts) % num_experts
        keys = jnp.where(slot_ids[:, 0] >= 0, place * src_slots + slot_ids[:, 0] - position * src_slots, -1)
        keys = jnp.swapaxes(keys, 1, 2)
        gates = jnp.swapaxes(gate_vals[:, 0], 1, 2)

        arrived = []
        combined = []
        weights = []
        for call_id, micros in enumerate(((0,), (1, 2), (3, 4, 5))):
            if combined:
                keys = lax.optimization_barrier((keys, combined[-1]))[0]
            rows = combine(micros, call_id, keys, gates, expert_out, residual, 512)
            combined.extend(rows)
            for micro, row in zip(micros, rows):
                arrived.append(lax.ppermute(row, 'pp', send_next))
            if call_id == 0:
                before = combined[-1]
                for wt in (w_query, w_key):
                    wt = lax.optimization_barrier((wt, before))[0]
                    before = regroup(position[None], wt, 256, 512)
                    weights.append(before)
                value_in = lax.optimization_barrier((w_value, before))[0]
                value_wt = regroup(None, value_in, 256, 512)
                for which in range(2):
                    weights.append(lax.ppermute(weights[which], 'ep', swap_pair))
                weights.append(value_wt)
                keys = lax.optimization_barrier((keys, value_wt))[0]

        flat_out = w_out[0].reshape(-1, d_model)
        result = None
        for micro in range(num_micro):
            rows = lax.optimization_barrier((arrived[0], combined[-1]))[0] if micro == 0 else arrived[micro]
            if micro:
                rows, result = lax.optimization_barrier((rows, result))
            result = attention(micro, rows, norm_w, weights, flat_out, result, residual.shape, 512)
        return result

    return jax.shard_map(device_step, mesh=mesh, in_specs=(tok_spec, tok_spec, tok_spec, tok_spec, tok_spec, P('pp', None), wt_spec, wt_spec, wt_spec, wt_spec), out_specs=tok_spec, check_vma=False)
```
